32 devices in a mesh: slab: 16 (over z, y, x), pencil: 2 (over core).
Axes of the slice: x: 2, y: 2, z: 4, core: 2. Of those that a mesh axis runs over, the one named last changes fastest.
Arguments:
- owner_map: int32 [16], replicated, may hold values from 0 to 15
- window_start: int32 [1], replicated, may hold values from 0 to 8
- child_maps: float32 [8, 20, 20], replicated, may hold values from -1 to 1
- innovation: float32 [20, 20], replicated, may hold values from -1.25 to 1.25
- coarse_bank: float32 [16, 20, 74898], P('slab'), may hold values from -6 to 6
- noise_middle: float32 [20, 64, 64, 128], P(None, 'slab', 'pencil'), may hold values from -6 to 6
- noise_finest: float32 [20, 128, 128, 256], P(None, 'slab', 'pencil'), may hold values from -6 to 6
Outputs:
- field_values: float32 [256, 256, 512], P('slab', 'pencil')
- zface_mean: float32 [128, 256, 512], P('slab', 'pencil')
- yface_mean: float32 [256, 128, 512], P('slab', 'pencil')
The draws below stay inside these ranges and needn't reach their ends.
All inputs are finite; a program needn't handle non-finite values.
Results may differ from the reference program's by a relative error of at most 0.0001.
Values sent between devices are 32-bit elements; how exact they have to be, the bound alone decides.
No kernel may reach another device: no remote copies, remote signals or barrier semaphores. Data moves between devices by JAX's collectives and lax.ppermute only.
A program may use at most 448 MiB of HBM per device.

```python
import math
import jax
import jax.numpy as jnp
import numpy as np
from jax import lax

K = 20
LEVELS = 8
ROOTS = 2
ROOTS_Z = 1
ROOTS_Y = 1
DEPTH = 16
COARSE = 74898
FZ = 128
FY = 128
FX = 256
N_SLAB = 16


def touch_ends(result, rng, least, top_value):
    spot = [jax.random.randint(jax.random.fold_in(rng, axis), (), 0, length) for axis, length in enumerate(result.shape)]
    widest = result.shape.index(max(result.shape))
    beside = spot[:widest] + [(spot[widest] + 1) % result.shape[widest]] + spot[widest + 1:]
    return result.at[tuple(spot)].set(least).at[tuple(beside)].set(top_value)


def steps_of(rng, dims, split, least, largest):
    level = 1.0
    for dim, shards_of in split:
        heights = jax.random.uniform(jax.random.fold_in(jax.random.fold_in(rng, 6), dim), (shards_of,), jnp.float32, least / len(split), largest / len(split))
        level = level * jnp.repeat(jnp.exp(heights), dims[dim] // shards_of).reshape((-1,) + (1,) * (len(dims) - 1 - dim))
    return level


def bell_draw(rng, shape, width, bound, cuts=(), kind=jnp.bfloat16):
    entries = width * jax.random.normal(rng, shape, jnp.float32)
    if cuts:
        entries = entries * steps_of(rng, shape, cuts, -0.22, 0.18)
    return jnp.clip(entries, -bound, bound).astype(kind)


def setup_inputs(seed: int = 0) -> dict:
    seeds = jax.random.split(jax.random.key(seed), 8)
    owner_map = touch_ends(jax.random.randint(seeds[0], (DEPTH,), 0, N_SLAB), jax.random.fold_in(seeds[0], 1), 0, N_SLAB - 1).astype(jnp.int32)
    window_start = jax.random.randint(seeds[1], (1,), 0, DEPTH - LEVELS + 1).astype(jnp.int32)
    child_maps = bell_draw(seeds[2], (8, K, K), (2 * K) ** -0.5, 1.0, (), jnp.float32)
    innovation = bell_draw(seeds[3], (K, K), K ** -0.5, 1.25, (), jnp.float32)
    coarse_bank = bell_draw(seeds[4], (N_SLAB, K, COARSE), 1.0, 6.0, ((0, 16),), jnp.float32)
    noise_middle = bell_draw(seeds[5], (K, FZ // 2, FY // 2, FX // 2), 1.0, 6.0, ((1, 16), (2, 2)), jnp.float32)
    noise_finest = bell_draw(seeds[6], (K, FZ, FY, FX), 1.0, 6.0, ((1, 16), (2, 2)), jnp.float32)
    return {"owner_map": owner_map, "window_start": window_start, "child_maps": child_maps, "innovation": innovation, "coarse_bank": coarse_bank, "noise_middle": noise_middle, "noise_finest": noise_finest}


def legendre(order, point):
    values = [1.0, point, 1.5 * point * point - 0.5, 2.5 * point * point * point - 1.5 * point]
    return values[order]

def basis_table(points):
    table_rows = []
    for point in points:
        w_coord, v_coord, u_coord = point
        entry = []
        for deg_x in range(4):
            for deg_y in range(4):
                for deg_z in range(4):
                    if deg_x + deg_y + deg_z <= 3:
                        factor = math.sqrt((2 * deg_x + 1) * (2 * deg_y + 1) * (2 * deg_z + 1))
                        entry.append(factor * legendre(deg_x, u_coord) * legendre(deg_y, v_coord) * legendre(deg_z, w_coord))
        table_rows.append(entry)
    return jnp.asarray(np.array(table_rows), jnp.float32)

def level_block(flat, level):
    scale = 2 ** level
    first = ROOTS_Z * ROOTS_Y * ROOTS
    offset = first * (8 ** level - 1) // 7
    length = first * 8 ** level
    return flat[:, offset:offset + length].reshape(flat.shape[0], ROOTS_Z * scale, ROOTS_Y * scale, ROOTS * scale)

def descend(parent, child_maps):
    kids = jnp.einsum('okn,nzyx->okzyx', child_maps, parent, precision=lax.Precision.HIGHEST)
    count, planes, rows_y, cols_x = parent.shape
    kids = kids.reshape(2, 2, 2, count, planes, rows_y, cols_x).transpose(3, 4, 0, 5, 1, 6, 2)
    return kids.reshape(count, 2 * planes, 2 * rows_y, 2 * cols_x)

def innovate(innovation, noise):
    return jnp.einsum('kn,nzyx->kzyx', innovation, noise, precision=lax.Precision.HIGHEST)

def expand(table, coeffs):
    return jnp.einsum('pk,kzyx->pzyx', table, coeffs, precision=lax.Precision.HIGHEST)

def reference(owner_map, window_start, child_maps, innovation, coarse_bank, noise_middle, noise_finest):
    coeffs = None
    for level in range(LEVELS - 2):
        owner = owner_map[window_start[0] + level].astype(jnp.int32)
        chosen = lax.dynamic_index_in_dim(coarse_bank, owner, 0, keepdims=False)
        fresh = innovate(innovation, level_block(chosen, level))
        coeffs = fresh if level == 0 else descend(coeffs, child_maps) + fresh
    coeffs = descend(coeffs, child_maps) + innovate(innovation, noise_middle)
    fine = descend(coeffs, child_maps) + innovate(innovation, noise_finest)
    count, planes, rows_y, cols_x = fine.shape
    halves = [-0.5, 0.5]
    inner = basis_table([(pz, py, px) for pz in halves for py in halves for px in halves])
    top = basis_table([(1.0, py, px) for py in halves for px in halves])
    bottom = basis_table([(-1.0, py, px) for py in halves for px in halves])
    north = basis_table([(pz, 1.0, px) for pz in halves for px in halves])
    south = basis_table([(pz, -1.0, px) for pz in halves for px in halves])
    values = expand(inner, fine).reshape(2, 2, 2, planes, rows_y, cols_x).transpose(3, 0, 4, 1, 5, 2)
    field_values = values.reshape(2 * planes, 2 * rows_y, 2 * cols_x)
    zsum = expand(top, fine) + jnp.roll(expand(bottom, fine), -1, axis=1)
    zface = (0.5 * zsum).reshape(2, 2, planes, rows_y, cols_x).transpose(2, 3, 0, 4, 1)
    zface_mean = zface.reshape(planes, 2 * rows_y, 2 * cols_x)
    ysum = expand(north, fine) + jnp.roll(expand(south, fine), -1, axis=2)
    yface = (0.5 * ysum).reshape(2, 2, planes, rows_y, cols_x).transpose(2, 0, 3, 4, 1)
    yface_mean = yface.reshape(2 * planes, rows_y, 2 * cols_x)
    return (field_values, zface_mean, yface_mean)
```

```python
import math

import jax
import jax.numpy as jnp
import numpy as np
from jax import lax
from jax.experimental import pallas as pl
from jax.experimental.pallas import tpu as pltpu
from jax.sharding import PartitionSpec as P

LEVELS = 8
ROOTS = 2
BANK = LEVELS - 2
LANES = 128
SUB = 8
HIGH = lax.Precision.HIGHEST


def legendre(order, point):
    values = [1.0, point, 1.5 * point * point - 0.5, 2.5 * point * point * point - 1.5 * point]
    return values[order]


def basis_row(pz, py, px):
    entry = []
    for deg_x in range(4):
        for deg_y in range(4):
            for deg_z in range(4):
                if deg_x + deg_y + deg_z <= 3:
                    factor = math.sqrt((2 * deg_x + 1) * (2 * deg_y + 1) * (2 * deg_z + 1))
                    entry.append(
                        factor * legendre(deg_x, px) * legendre(deg_y, py) * legendre(deg_z, pz)
                    )
    return entry


def fine_layout():
    halves = [-0.5, 0.5]
    table, index = [], {}

    def functional(key, row):
        if key not in index:
            index[key] = len(table)
            table.append(row)
        return index[key]

    rows = []
    for px in halves:
        for pz in halves:
            for y2 in range(2 * SUB):
                py = halves[y2 % 2]
                rows.append([(y2 // 2, functional((pz, py, px), basis_row(pz, py, px)))])
        for w in (1.0, -1.0):
            for y2 in range(2 * SUB):
                py = halves[y2 % 2]
                half_row = [0.5 * v for v in basis_row(w, py, px)]
                rows.append([(y2 // 2, functional((w, py, px), half_row))])
        for pz in halves:
            north = functional((pz, 1.0, px), [0.5 * v for v in basis_row(pz, 1.0, px)])
            south = functional((pz, -1.0, px), [0.5 * v for v in basis_row(pz, -1.0, px)])
            for y in range(SUB):
                row = [(y, north)]
                if y + 1 < SUB:
                    row.append((y + 1, south))
                rows.append(row)
        for pz in halves:
            south = functional((pz, -1.0, px), [0.5 * v for v in basis_row(pz, -1.0, px)])
            for y in range(SUB):
                rows.append([(0, south)] if y == SUB - 1 else [])
    return np.array(table, np.float32), rows


def selector(rows, functionals):
    chosen = np.zeros((len(rows), SUB, functionals), np.float32)
    for r, terms in enumerate(rows):
        for y, f in terms:
            chosen[r, y, f] = 1.0
    return chosen


def left_factors(maps, chosen):
    m, _, f = chosen.shape
    k = maps.shape[2]
    own = jnp.einsum("ryf,fn->rny", chosen, maps[0], precision=HIGH).reshape(1, m, k * SUB)
    pairs = chosen.reshape(m, SUB // 2, 2, f)
    octants = maps[1:].reshape(2, 2, 2, f, k)
    par = jnp.einsum("rqyf,zyxfn->zrnxq", pairs, octants, precision=HIGH).reshape(2, m, k * SUB)
    return jnp.concatenate([own, par], axis=0)


class Plan:
    def __init__(self, mid_planes, mid_rows, slabs, pencils):
        self.slabs, self.pencils = slabs, pencils
        self.mid_planes, self.mid_rows = mid_planes, mid_rows
        self.w, self.r, self.x, self.n, self.off, self.place = [], [], [], [], [], []
        for j in range(BANK):
            self.w.append(max(1, mid_planes >> (BANK - j)))
            self.r.append(max(1, mid_rows >> (BANK - j)))
            self.x.append(ROOTS << j)
            self.n.append(self.w[j] * self.r[j] * self.x[j])
            self.off.append(ROOTS * (8**j - 1) // 7)
        self.big = [j for j in range(BANK) if self.r[j] * self.x[j] % LANES == 0]
        self.small = [j for j in range(BANK) if j not in self.big]
        lane = 0
        self.place = [0] * BANK
        for j in reversed(self.big):
            self.place[j] = lane
            lane += self.n[j]
        self.small_at = lane
        for j in reversed(self.small):
            assert self.w[j] == 1
            self.place[j] = lane
            lane += self.n[j]
        assert lane - self.small_at <= LANES
        self.chunks = (self.small_at + LANES) // LANES

    def z0(self, j, slab):
        return (slab * self.mid_planes) >> (BANK - j)

    def y0(self, j, pencil):
        return (pencil * self.mid_rows) >> (BANK - j)


def pack_kernel(plan, where_ref, bank_ref, out_ref):
    slab = pl.program_id(0)
    pencil = where_ref[0]
    k = bank_ref.shape[1]

    def put(chunk, value):
        out_ref[0, chunk * k : (chunk + 1) * k, :] = value

    for j in plan.big:
        rows = 2**j
        length = plan.r[j] * plan.x[j]
        base = plan.off[j] // LANES * LANES
        delta = plan.off[j] - base
        for plane in range(plan.w[j]):
            start = (plan.z0(j, slab) + plane) * rows * plan.x[j] + plan.y0(j, pencil) * plan.x[j]
            start = pl.multiple_of(base + start, LANES)
            wide = bank_ref[0, :, pl.ds(start, length + LANES)]
            if delta:
                wide = pltpu.roll(wide, length + LANES - delta, 1)
            at = (plan.place[j] + plane * length) // LANES
            for c in range(length // LANES):
                put(at + c, wide[:, c * LANES : (c + 1) * LANES])
    lane = lax.broadcasted_iota(jnp.int32, (k, LANES), 1)
    small = jnp.zeros((k, LANES), jnp.float32)
    for j in plan.small:
        base = plan.off[j] // LANES * LANES
        end = -(-(plan.off[j] + ROOTS * 8**j) // LANES) * LANES
        size = end - base
        start = plan.off[j] - base
        start = start + (plan.z0(j, slab) * 2**j + plan.y0(j, pencil)) * plan.x[j]
        at = plan.place[j] - plan.small_at
        shift = lax.rem(at - start + 2 * size, size)
        moved = pltpu.roll(bank_ref[0, :, base:end], shift, 1)[:, :LANES]
        small = jnp.where((lane >= at) & (lane < at + plan.n[j]), moved, small)
    put(plan.small_at // LANES, small)


def split3(value):
    hi = value.astype(jnp.bfloat16)
    rest = value - hi.astype(jnp.float32)
    mid = rest.astype(jnp.bfloat16)
    lo = (rest - mid.astype(jnp.float32)).astype(jnp.bfloat16)
    return hi, mid, lo


def split2(value):
    hi = value.astype(jnp.bfloat16)
    lo = (value - hi.astype(jnp.float32)).astype(jnp.bfloat16)
    return hi, lo


def dot(left, right):
    return lax.dot_general(
        left, right, (((1,), (0,)), ((), ())), preferred_element_type=jnp.float32
    )


def coarse_kernel(plan, k, ints_ref, recv_ref, left_ref, out_ref):
    kp = 24
    lh, ll = split2(left_ref[...])
    left = jnp.concatenate([lh, lh, ll], axis=1)

    def chunk_of(j, c):
        return recv_ref[ints_ref[j], c * k : (c + 1) * k, :]

    coeffs = None
    for j in range(BANK):
        n = max(LANES, plan.n[j])
        if j in plan.small:
            at = plan.place[j] - plan.small_at
            noise = chunk_of(j, plan.small_at // LANES)
            if at:
                noise = pltpu.roll(noise, LANES - at, 1)
        else:
            first = plan.place[j] // LANES
            noise = jnp.concatenate([chunk_of(j, first + c) for c in range(n // LANES)], axis=1)
        noise = jnp.concatenate([noise, jnp.zeros((kp - k, n), jnp.float32)], axis=0)
        pieces = []
        if j == 0:
            pieces = [jnp.zeros((8 * kp, n), jnp.float32)]
        else:
            lane = lax.broadcasted_iota(jnp.int32, (1, n), 1)
            x = lane & (plan.x[j] - 1)
            row = (lane // plan.x[j]) & (plan.r[j] - 1)
            plane = lane // (plan.x[j] * plan.r[j])
            y_odd = (row & 1) if plan.r[j] > 1 else ints_ref[2 * BANK + j]
            z_odd = (plane & 1) if plan.w[j] > 1 else ints_ref[BANK + j]
            octant = 4 * z_odd + 2 * y_odd + (x & 1)
            parent = ((plane // 2) * plan.r[j - 1] + row // 2) * plan.x[j - 1] + x // 2
            parents = coeffs.shape[1]
            spot = lax.broadcasted_iota(jnp.int32, (parents, n), 0)
            onehot = jnp.where(spot == parent, 1.0, 0.0).astype(jnp.bfloat16)
            parts = jnp.concatenate([p.astype(jnp.float32) for p in split3(coeffs)], axis=0)
            up = dot(parts.astype(jnp.bfloat16), onehot)
            up = up[:kp] + up[kp : 2 * kp] + up[2 * kp :]
            pieces = [jnp.where(octant == o, up, 0.0) for o in range(8)]
        right = jnp.concatenate(pieces + [noise], axis=0)
        rh, rl = split2(right)
        coeffs = dot(left, jnp.concatenate([rh, rl, rh], axis=0))
    out_ref[...] = coeffs


def lift(block, sources, half):
    k = block.shape[0]
    flat = block.reshape(k * SUB, LANES)
    lane = lax.broadcasted_iota(jnp.int32, (k * SUB, LANES), 1)
    row = lax.broadcasted_iota(jnp.int32, (k, SUB, LANES), 1)
    even = (lax.broadcasted_iota(jnp.int32, (k, SUB, LANES), 2) & 1) == 0
    low = row < SUB // 2
    wide = []
    for c in range(sources):
        up = jnp.take_along_axis(
            flat, lane // 2 + c * (LANES // 2), axis=1, mode="promise_in_bounds"
        ).reshape(k, SUB, LANES)
        turned = pltpu.roll(up, SUB // 2, 1)
        both = jnp.where(low, up, turned) if half == 0 else jnp.where(low, turned, up)
        wide.append(jnp.where(low == even, both, 0.0).reshape(k * SUB, LANES))
    return jnp.concatenate(wide, axis=1) if sources > 1 else wide[0]


def operand(noise, raised):
    nh, nl = split2(noise)
    ph, pl_ = split2(raised)
    return jnp.concatenate([nh, nl, nh, ph, pl_, ph], axis=0)


def fine_kernel(
    ints_ref, mid_left, fine_left, upper, noise_mid, noise, field, zface, yface, zfirst, sfirst,
    mid, mid_s, fine_s, zcarry,
):
    step = pl.program_id(0)
    steps = pl.num_programs(0)
    plane = steps - 1 - step
    k = noise.shape[0]
    rows, cols = noise.shape[2], noise.shape[3]
    mid_planes, mid_rows, mid_cols = noise_mid.shape[1:]

    @pl.when(step == 0)
    def _():
        for source, target in ((mid_left, mid_s), (fine_left, fine_s)):
            wh, wl = split2(source[0])
            for oz in range(2):
                vh, vl = split2(source[1 + oz])
                target[oz] = jnp.concatenate([wh, wh, wl, vh, vh, vl], axis=1)
        for z in range(mid_planes):
            left = mid_s[(ints_ref[0] + z) % 2]
            for yb in range(mid_rows // 16):
                parent = upper[:, z // 2, yb * SUB : (yb + 1) * SUB, :]
                for half in range(2):
                    y = yb * 16 + half * SUB
                    own = noise_mid[:, z, y : y + SUB, :].reshape(k * SUB, mid_cols)
                    got = dot(left, operand(own, lift(parent, 1, half)))
                    mid[:, z, y : y + SUB, :] = got.reshape(k, SUB, mid_cols)
        zcarry[...] = jnp.zeros(zcarry.shape, jnp.float32)

    left = fine_s[plane % 2]
    group = left.shape[0] // 2
    sources = cols // LANES
    lane = lax.broadcasted_iota(jnp.int32, (group, LANES), 1)
    even = (lane & 1) == 0
    south = [jnp.zeros((2 * SUB, LANES), jnp.float32) for _ in range(2 * sources)]
    for yb in reversed(range(rows // 16)):
        parent = mid[:, plane // 2, yb * SUB : (yb + 1) * SUB, :]
        for half in (1, 0):
            y = yb * 16 + half * SUB
            own = noise[:, 0, y : y + SUB, :].reshape(k * SUB, cols)
            got = dot(left, operand(own, lift(parent, sources, half)))
            for c in range(2 * sources):
                s = c // 2
                index = lane // 2 + (c % 2) * (LANES // 2)
                span = slice(s * LANES, (s + 1) * LANES)
                a = jnp.take_along_axis(
                    got[:group, span], index, axis=1, mode="promise_in_bounds"
                )
                b = jnp.take_along_axis(
                    got[group:, span], index, axis=1, mode="promise_in_bounds"
                )
                out = jnp.where(even, a, b)
                to = slice(c * LANES, (c + 1) * LANES)
                y2 = slice(2 * y, 2 * y + 16)
                field[0, y2, to] = out[0:16]
                field[1, y2, to] = out[16:32]
                zface[0, y2, to] = out[32:48] + zcarry[y2, to]
                zcarry[y2, to] = out[48:64]
                faces = out[64:80] + south[c]
                yface[0, y : y + SUB, to] = faces[:SUB]
                yface[1, y : y + SUB, to] = faces[SUB:]
                south[c] = out[80:96]
    for c in range(2 * sources):
        to = slice(c * LANES, (c + 1) * LANES)
        sfirst[0, :, to] = south[c]

    @pl.when(plane == 0)
    def _():
        zfirst[...] = zcarry[...]


def shards(
    owner_map, window_start, child_maps, innovation, coarse_bank, noise_middle, noise_finest
):
    slabs, pencils = lax.axis_size("slab"), lax.axis_size("pencil")
    slab, pencil = lax.axis_index("slab"), lax.axis_index("pencil")
    k, mid_planes, mid_rows, mid_cols = noise_middle.shape
    _, planes, rows, cols = noise_finest.shape
    plan = Plan(mid_planes, mid_rows, slabs, pencils)
    f32 = jnp.float32
    smem = pl.BlockSpec(memory_space=pltpu.SMEM)

    def whole(shape):
        return pl.BlockSpec(shape, lambda *_: (0,) * len(shape))

    packed_rows = plan.chunks * k
    packed = pl.pallas_call(
        lambda *refs: pack_kernel(plan, *refs),
        grid=(slabs,),
        in_specs=[smem, whole((1, k, -(-coarse_bank.shape[2] // LANES) * LANES))],
        out_specs=pl.BlockSpec((1, packed_rows, LANES), lambda s: (s, 0, 0)),
        out_shape=jax.ShapeDtypeStruct((slabs, packed_rows, LANES), f32),
        compiler_params=pltpu.CompilerParams(vmem_limit_bytes=48 << 20),
        name="pack",
    )(pencil.reshape(1).astype(jnp.int32), coarse_bank)
    recv = lax.all_to_all(packed, "slab", 0, 0, tiled=True)

    table, fine_rows = fine_layout()
    maps = jnp.concatenate([innovation[None], child_maps], axis=0)
    fine_maps = jnp.einsum("fk,mkn->mfn", jnp.asarray(table), maps, precision=HIGH)
    fine_left = left_factors(fine_maps, selector(fine_rows, table.shape[0]))
    mid_left = left_factors(maps, selector([[(y, o)] for o in range(k) for y in range(SUB)], k))
    owners = lax.dynamic_slice(owner_map, (window_start[0],), (BANK,))
    z_odd = jnp.stack([plan.z0(j, slab) % 2 for j in range(BANK)])
    y_odd = jnp.stack([plan.y0(j, pencil) % 2 for j in range(BANK)])
    ints = jnp.concatenate([owners, z_odd, y_odd]).astype(jnp.int32)
    coarse_left = jnp.concatenate([child_maps, innovation[None]], axis=0)
    coarse_left = jnp.pad(coarse_left, ((0, 0), (0, 24 - k), (0, 24 - k)))
    coarse_left = coarse_left.transpose(1, 0, 2).reshape(24, 9 * 24)

    last = BANK - 1
    upper = pl.pallas_call(
        lambda *refs: coarse_kernel(plan, k, *refs),
        in_specs=[smem, pl.BlockSpec(memory_space=pltpu.VMEM), pl.BlockSpec(memory_space=pltpu.VMEM)],
        out_specs=pl.BlockSpec(memory_space=pltpu.VMEM),
        out_shape=jax.ShapeDtypeStruct((24, plan.n[last]), f32),
        compiler_params=pltpu.CompilerParams(vmem_limit_bytes=48 << 20),
        name="coarse",
    )(ints, recv, coarse_left)
    upper = upper[:k].reshape(k, plan.w[last], plan.r[last], plan.x[last])
    upper = jnp.pad(upper, ((0, 0), (0, 0), (0, 0), (0, LANES - plan.x[last])))

    m_fine = fine_left.shape[1]
    depth = 6 * k * SUB
    flip = planes - 1
    field, zface, yface, zfirst, sfirst = pl.pallas_call(
        fine_kernel,
        grid=(planes,),
        in_specs=[
            smem,
            whole(mid_left.shape),
            whole(fine_left.shape),
            whole(upper.shape),
            whole(noise_middle.shape),
            pl.BlockSpec((k, 1, rows, cols), lambda i: (0, flip - i, 0, 0)),
        ],
        out_specs=[
            pl.BlockSpec((2, 2 * rows, 2 * cols), lambda i: (flip - i, 0, 0)),
            pl.BlockSpec((1, 2 * rows, 2 * cols), lambda i: (flip - i, 0, 0)),
            pl.BlockSpec((2, rows, 2 * cols), lambda i: (flip - i, 0, 0)),
            whole((2 * rows, 2 * cols)),
            pl.BlockSpec((1, 2 * SUB, 2 * cols), lambda i: (flip - i, 0, 0)),
        ],
        out_shape=[
            jax.ShapeDtypeStruct((2 * planes, 2 * rows, 2 * cols), f32),
            jax.ShapeDtypeStruct((planes, 2 * rows, 2 * cols), f32),
            jax.ShapeDtypeStruct((2 * planes, rows, 2 * cols), f32),
            jax.ShapeDtypeStruct((2 * rows, 2 * cols), f32),
            jax.ShapeDtypeStruct((planes, 2 * SUB, 2 * cols), f32),
        ],
        scratch_shapes=[
            pltpu.VMEM((k, mid_planes, mid_rows, mid_cols), f32),
            pltpu.VMEM((2, mid_left.shape[1], depth), jnp.bfloat16),
            pltpu.VMEM((2, m_fine, depth), jnp.bfloat16),
            pltpu.VMEM((2 * rows, 2 * cols), f32),
        ],
        compiler_params=pltpu.CompilerParams(
            dimension_semantics=("arbitrary",), vmem_limit_bytes=52 << 20
        ),
        name="fine",
    )(
        (slab * mid_planes % 2).reshape(1).astype(jnp.int32),
        mid_left, fine_left, upper, noise_middle, noise_finest,
    )

    above = lax.ppermute(zfirst, "slab", [((i + 1) % slabs, i) for i in range(slabs)])
    edge = sfirst.reshape(2 * planes, SUB, 2 * cols)[:, SUB - 1]
    beside = lax.ppermute(edge, "pencil", [((i + 1) % pencils, i) for i in range(pencils)])
    zface = zface.at[planes - 1].add(above)
    yface = yface.at[:, rows - 1].add(beside)
    return (field, zface, yface)


def solution(mesh):
    placed = (
        P(),
        P(),
        P(),
        P(),
        P("slab", None, None),
        P(None, "slab", "pencil", None),
        P(None, "slab", "pencil", None),
    )
    return jax.shard_map(
        shards,
        mesh=mesh,
        in_specs=placed,
        out_specs=(P("slab", "pencil", None), P("slab", "pencil", None), P("slab", "pencil", None)),
        check_vma=False,
    )
```

```python
import math

import jax
import jax.numpy as jnp
import numpy as np
from jax import lax
from jax.experimental import pallas as pl
from jax.experimental.pallas import tpu as pltpu
from jax.sharding import PartitionSpec as P

LEVELS = 8
ROOTS = 2
BANK = LEVELS - 2
LANES = 128
SUB = 8
HIGH = lax.Precision.HIGHEST


def legendre(order, point):
    values = [1.0, point, 1.5 * point * point - 0.5, 2.5 * point * point * point - 1.5 * point]
    return values[order]


def basis_row(pz, py, px):
    entry = []
    for deg_x in range(4):
        for deg_y in range(4):
            for deg_z in range(4):
                if deg_x + deg_y + deg_z <= 3:
                    factor = math.sqrt((2 * deg_x + 1) * (2 * deg_y + 1) * (2 * deg_z + 1))
                    entry.append(
                        factor * legendre(deg_x, px) * legendre(deg_y, py) * legendre(deg_z, pz)
                    )
    return entry


def fine_layout():
    halves = [-0.5, 0.5]
    table, index = [], {}

    def functional(key, row):
        if key not in index:
            index[key] = len(table)
            table.append(row)
        return index[key]

    rows = []
    for px in halves:
        for pz in halves:
            for y2 in range(2 * SUB):
                py = halves[y2 % 2]
                rows.append([(y2 // 2, functional((pz, py, px), basis_row(pz, py, px)))])
        for w in (1.0, -1.0):
            for y2 in range(2 * SUB):
                py = halves[y2 % 2]
                half_row = [0.5 * v for v in basis_row(w, py, px)]
                rows.append([(y2 // 2, functional((w, py, px), half_row))])
        for pz in halves:
            north = functional((pz, 1.0, px), [0.5 * v for v in basis_row(pz, 1.0, px)])
            south = functional((pz, -1.0, px), [0.5 * v for v in basis_row(pz, -1.0, px)])
            for y in range(SUB):
                row = [(y, north)]
                if y + 1 < SUB:
                    row.append((y + 1, south))
                rows.append(row)
        for pz in halves:
            south = functional((pz, -1.0, px), [0.5 * v for v in basis_row(pz, -1.0, px)])
            for y in range(SUB):
                rows.append([(0, south)] if y == SUB - 1 else [])
    return np.array(table, np.float32), rows


def selector(rows, functionals):
    chosen = np.zeros((len(rows), SUB, functionals), np.float32)
    for r, terms in enumerate(rows):
        for y, f in terms:
            chosen[r, y, f] = 1.0
    return chosen


def left_factors(maps, chosen):
    m, _, f = chosen.shape
    k = maps.shape[2]
    own = jnp.einsum("ryf,fn->rny", chosen, maps[0], precision=HIGH).reshape(1, m, k * SUB)
    pairs = chosen.reshape(m, SUB // 2, 2, f)
    octants = maps[1:].reshape(2, 2, 2, f, k)
    par = jnp.einsum("rqyf,zyxfn->zrnxq", pairs, octants, precision=HIGH).reshape(2, m, k * SUB)
    return jnp.concatenate([own, par], axis=0)


class Plan:
    def __init__(self, mid_planes, mid_rows, slabs, pencils):
        self.slabs, self.pencils = slabs, pencils
        self.mid_planes, self.mid_rows = mid_planes, mid_rows
        self.w, self.r, self.x, self.n, self.off, self.place = [], [], [], [], [], []
        for j in range(BANK):
            self.w.append(max(1, mid_planes >> (BANK - j)))
            self.r.append(max(1, mid_rows >> (BANK - j)))
            self.x.append(ROOTS << j)
            self.n.append(self.w[j] * self.r[j] * self.x[j])
            self.off.append(ROOTS * (8**j - 1) // 7)
        self.big = [j for j in range(BANK) if self.r[j] * self.x[j] % LANES == 0]
        self.small = [j for j in range(BANK) if j not in self.big]
        lane = 0
        self.place = [0] * BANK
        for j in reversed(self.big):
            self.place[j] = lane
            lane += self.n[j]
        self.small_at = lane
        for j in reversed(self.small):
            assert self.w[j] == 1
            self.place[j] = lane
            lane += self.n[j]
        assert lane - self.small_at <= LANES
        self.chunks = (self.small_at + LANES) // LANES
        third = max(1, self.chunks * 3 // 8)
        self.parts = [third, third, self.chunks - 2 * third]

    def part_of(self, chunk):
        for part, count in enumerate(self.parts):
            if chunk < count:
                return part, chunk
            chunk -= count

    def z0(self, j, slab):
        return (slab * self.mid_planes) >> (BANK - j)

    def y0(self, j, pencil):
        return (pencil * self.mid_rows) >> (BANK - j)


def pack_kernel(plan, k, where_ref, bank_ref, *out_refs):
    slab = pl.program_id(0)
    pencil = where_ref[0]

    def put(chunk, value):
        part, at = plan.part_of(chunk)
        out_refs[part][0, at * k : (at + 1) * k, :] = value

    for j in plan.big:
        rows = 2**j
        length = plan.r[j] * plan.x[j]
        base = plan.off[j] // LANES * LANES
        delta = plan.off[j] - base
        for plane in range(plan.w[j]):
            start = (plan.z0(j, slab) + plane) * rows * plan.x[j] + plan.y0(j, pencil) * plan.x[j]
            start = pl.multiple_of(base + start, LANES)
            wide = bank_ref[0, :, pl.ds(start, length + LANES)]
            if delta:
                wide = pltpu.roll(wide, length + LANES - delta, 1)
            at = (plan.place[j] + plane * length) // LANES
            for c in range(length // LANES):
                put(at + c, jnp.where(where_ref[1 + j] > 0, wide[:, c * LANES : (c + 1) * LANES], 0.0))
    lane = lax.broadcasted_iota(jnp.int32, (k, LANES), 1)
    small = jnp.zeros((k, LANES), jnp.float32)
    for j in plan.small:
        base = plan.off[j] // LANES * LANES
        end = -(-(plan.off[j] + ROOTS * 8**j) // LANES) * LANES
        size = end - base
        start = plan.off[j] - base
        start = start + (plan.z0(j, slab) * 2**j + plan.y0(j, pencil)) * plan.x[j]
        at = plan.place[j] - plan.small_at
        shift = lax.rem(at - start + 2 * size, size)
        moved = pltpu.roll(bank_ref[0, :, base:end], shift, 1)[:, :LANES]
        moved = jnp.where(where_ref[1 + j] > 0, moved, 0.0)
        small = jnp.where((lane >= at) & (lane < at + plan.n[j]), moved, small)
    put(plan.small_at // LANES, small)


def split3(value):
    hi = value.astype(jnp.bfloat16)
    rest = value - hi.astype(jnp.float32)
    mid = rest.astype(jnp.bfloat16)
    lo = (rest - mid.astype(jnp.float32)).astype(jnp.bfloat16)
    return hi, mid, lo


def split2(value):
    hi = value.astype(jnp.bfloat16)
    lo = (value - hi.astype(jnp.float32)).astype(jnp.bfloat16)
    return hi, lo


def dot(left, right):
    return lax.dot_general(
        left, right, (((1,), (0,)), ((), ())), preferred_element_type=jnp.float32
    )


def coarse_kernel(plan, k, ints_ref, recv_a, recv_b, recv_c, left_ref, out_ref):
    kp = 24
    lh, ll = split2(left_ref[...])
    left = jnp.concatenate([lh, lh, ll], axis=1)

    def chunk_of(c):
        part, at = plan.part_of(c)
        return (recv_a, recv_b, recv_c)[part][at * k : (at + 1) * k, :]

    coeffs = None
    for j in range(BANK):
        n = max(LANES, plan.n[j])
        if j in plan.small:
            at = plan.place[j] - plan.small_at
            noise = chunk_of(plan.small_at // LANES)
            if at:
                noise = pltpu.roll(noise, LANES - at, 1)
        else:
            first = plan.place[j] // LANES
            noise = jnp.concatenate([chunk_of(first + c) for c in range(n // LANES)], axis=1)
        noise = jnp.concatenate([noise, jnp.zeros((kp - k, n), jnp.float32)], axis=0)
        pieces = []
        if j == 0:
            pieces = [jnp.zeros((8 * kp, n), jnp.float32)]
        else:
            lane = lax.broadcasted_iota(jnp.int32, (1, n), 1)
            x = lane & (plan.x[j] - 1)
            row = (lane // plan.x[j]) & (plan.r[j] - 1)
            plane = lane // (plan.x[j] * plan.r[j])
            y_odd = (row & 1) if plan.r[j] > 1 else ints_ref[BANK + j]
            z_odd = (plane & 1) if plan.w[j] > 1 else ints_ref[j]
            octant = 4 * z_odd + 2 * y_odd + (x & 1)
            parent = ((plane // 2) * plan.r[j - 1] + row // 2) * plan.x[j - 1] + x // 2
            parents = coeffs.shape[1]
            spot = lax.broadcasted_iota(jnp.int32, (parents, n), 0)
            onehot = jnp.where(spot == parent, 1.0, 0.0).astype(jnp.bfloat16)
            parts = jnp.concatenate([p.astype(jnp.float32) for p in split3(coeffs)], axis=0)
            up = dot(parts.astype(jnp.bfloat16), onehot)
            up = up[:kp] + up[kp : 2 * kp] + up[2 * kp :]
            pieces = [jnp.where(octant == o, up, 0.0) for o in range(8)]
        right = jnp.concatenate(pieces + [noise], axis=0)
        rh, rl = split2(right)
        coeffs = dot(left, jnp.concatenate([rh, rl, rh], axis=0))
    out_ref[...] = coeffs


def lift(block, sources, half):
    k = block.shape[0]
    flat = block.reshape(k * SUB, LANES)
    lane = lax.broadcasted_iota(jnp.int32, (k * SUB, LANES), 1)
    row = lax.broadcasted_iota(jnp.int32, (k, SUB, LANES), 1)
    even = (lax.broadcasted_iota(jnp.int32, (k, SUB, LANES), 2) & 1) == 0
    low = row < SUB // 2
    wide = []
    for c in range(sources):
        up = jnp.take_along_axis(
            flat, lane // 2 + c * (LANES // 2), axis=1, mode="promise_in_bounds"
        ).reshape(k, SUB, LANES)
        turned = pltpu.roll(up, SUB // 2, 1)
        both = jnp.where(low, up, turned) if half == 0 else jnp.where(low, turned, up)
        wide.append(jnp.where(low == even, both, 0.0).reshape(k * SUB, LANES))
    return jnp.concatenate(wide, axis=1) if sources > 1 else wide[0]


def operand(noise, raised):
    nh, nl = split2(noise)
    ph, pl_ = split2(raised)
    return jnp.concatenate([nh, nl, nh, ph, pl_, ph], axis=0)


def fine_kernel(
    ints_ref, mid_left, fine_left, upper, noise_mid, noise, field, zface, yface, zfirst, sfirst,
    mid, mid_s, fine_s, zcarry,
):
    step = pl.program_id(0)
    steps = pl.num_programs(0)
    plane = steps - 1 - step
    k = noise.shape[0]
    rows, cols = noise.shape[2], noise.shape[3]
    mid_planes, mid_rows, mid_cols = noise_mid.shape[1:]

    @pl.when(step == 0)
    def _():
        for source, target in ((mid_left, mid_s), (fine_left, fine_s)):
            wh, wl = split2(source[0])
            for oz in range(2):
                vh, vl = split2(source[1 + oz])
                target[oz] = jnp.concatenate([wh, wh, wl, vh, vh, vl], axis=1)
        for z in range(mid_planes):
            left = mid_s[(ints_ref[0] + z) % 2]
            for yb in range(mid_rows // 16):
                parent = upper[:, z // 2, yb * SUB : (yb + 1) * SUB, :]
                for half in range(2):
                    y = yb * 16 + half * SUB
                    own = noise_mid[:, z, y : y + SUB, :].reshape(k * SUB, mid_cols)
                    got = dot(left, operand(own, lift(parent, 1, half)))
                    mid[:, z, y : y + SUB, :] = got.reshape(k, SUB, mid_cols)
        zcarry[...] = jnp.zeros(zcarry.shape, jnp.float32)

    left = fine_s[plane % 2]
    group = left.shape[0] // 2
    sources = cols // LANES
    lane = lax.broadcasted_iota(jnp.int32, (group, LANES), 1)
    even = (lane & 1) == 0
    south = [jnp.zeros((2 * SUB, LANES), jnp.float32) for _ in range(2 * sources)]
    for yb in reversed(range(rows // 16)):
        parent = mid[:, plane // 2, yb * SUB : (yb + 1) * SUB, :]
        for half in (1, 0):
            y = yb * 16 + half * SUB
            own = noise[:, 0, y : y + SUB, :].reshape(k * SUB, cols)
            got = dot(left, operand(own, lift(parent, sources, half)))
            for c in range(2 * sources):
                s = c // 2
                index = lane // 2 + (c % 2) * (LANES // 2)
                span = slice(s * LANES, (s + 1) * LANES)
                a = jnp.take_along_axis(
                    got[:group, span], index, axis=1, mode="promise_in_bounds"
                )
                b = jnp.take_along_axis(
                    got[group:, span], index, axis=1, mode="promise_in_bounds"
                )
                out = jnp.where(even, a, b)
                to = slice(c * LANES, (c + 1) * LANES)
                y2 = slice(2 * y, 2 * y + 16)
                field[0, y2, to] = out[0:16]
                field[1, y2, to] = out[16:32]
                zface[0, y2, to] = out[32:48] + zcarry[y2, to]
                zcarry[y2, to] = out[48:64]
                faces = out[64:80] + south[c]
                yface[0, y : y + SUB, to] = faces[:SUB]
                yface[1, y : y + SUB, to] = faces[SUB:]
                south[c] = out[80:96]
    for c in range(2 * sources):
        to = slice(c * LANES, (c + 1) * LANES)
        sfirst[0, :, to] = south[c]

    @pl.when(plane == 0)
    def _():
        zfirst[...] = zcarry[...]


def scatter_windows(packed, slabs):
    sizes = {"z": (slabs // 4, 4), "y": (2, 2), "x": (2, 1)}
    parts = [p.reshape((slabs // 4, 2, 2) + p.shape[1:]) for p in packed]
    left = [["z", "y", "x"] for _ in parts]
    slab = lax.axis_index("slab")
    for stage in range(3):
        keep, send, routes, home = [], [], [], []
        for i, order in enumerate(("xyz", "yzx", "zxy")):
            size, stride = sizes[order[stage]]
            axis = left[i].index(order[stage])
            left[i].remove(order[stage])
            me = (slab // stride) % size
            keep.append(lax.dynamic_index_in_dim(parts[i], me, axis, False))
            for hop in range(1, size):
                send.append(lax.dynamic_index_in_dim(parts[i], (me + hop) % size, axis, False))
                route = []
                for d in range(slabs):
                    at = (d // stride) % size
                    route.append((d, d + ((at + hop) % size - at) * stride))
                routes.append(route)
                home.append(i)
        send = lax.optimization_barrier(tuple(send))
        got = [lax.ppermute(piece, "slab", route) for piece, route in zip(send, routes)]
        got = lax.optimization_barrier(tuple(got))
        for i, piece in zip(home, got):
            keep[i] = keep[i] + piece
        parts = keep
    return parts


def shards(
    owner_map, window_start, child_maps, innovation, coarse_bank, noise_middle, noise_finest
):
    slabs, pencils = lax.axis_size("slab"), lax.axis_size("pencil")
    slab, pencil = lax.axis_index("slab"), lax.axis_index("pencil")
    k, mid_planes, mid_rows, mid_cols = noise_middle.shape
    _, planes, rows, cols = noise_finest.shape
    plan = Plan(mid_planes, mid_rows, slabs, pencils)
    f32 = jnp.float32
    smem = pl.BlockSpec(memory_space=pltpu.SMEM)

    def whole(shape):
        return pl.BlockSpec(shape, lambda *_: (0,) * len(shape))

    owners = lax.dynamic_slice(owner_map, (window_start[0],), (BANK,))
    held = (owners == slab).astype(jnp.int32)
    packed = pl.pallas_call(
        lambda *refs: pack_kernel(plan, k, *refs),
        grid=(slabs,),
        in_specs=[smem, whole((1, k, -(-coarse_bank.shape[2] // LANES) * LANES))],
        out_specs=[pl.BlockSpec((1, c * k, LANES), lambda s: (s, 0, 0)) for c in plan.parts],
        out_shape=[jax.ShapeDtypeStruct((slabs, c * k, LANES), f32) for c in plan.parts],
        compiler_params=pltpu.CompilerParams(vmem_limit_bytes=48 << 20),
        name="pack",
    )(jnp.concatenate([pencil.reshape(1).astype(jnp.int32), held]), coarse_bank)
    recv = scatter_windows(packed, slabs)

    table, fine_rows = fine_layout()
    maps = jnp.concatenate([innovation[None], child_maps], axis=0)
    fine_maps = jnp.einsum("fk,mkn->mfn", jnp.asarray(table), maps, precision=HIGH)
    fine_left = left_factors(fine_maps, selector(fine_rows, table.shape[0]))
    mid_left = left_factors(maps, selector([[(y, o)] for o in range(k) for y in range(SUB)], k))
    z_odd = jnp.stack([plan.z0(j, slab) % 2 for j in range(BANK)])
    y_odd = jnp.stack([plan.y0(j, pencil) % 2 for j in range(BANK)])
    ints = jnp.concatenate([z_odd, y_odd]).astype(jnp.int32)
    coarse_left = jnp.concatenate([child_maps, innovation[None]], axis=0)
    coarse_left = jnp.pad(coarse_left, ((0, 0), (0, 24 - k), (0, 24 - k)))
    coarse_left = coarse_left.transpose(1, 0, 2).reshape(24, 9 * 24)

    last = BANK - 1
    upper = pl.pallas_call(
        lambda *refs: coarse_kernel(plan, k, *refs),
        in_specs=[smem] + [pl.BlockSpec(memory_space=pltpu.VMEM)] * 4,
        out_specs=pl.BlockSpec(memory_space=pltpu.VMEM),
        out_shape=jax.ShapeDtypeStruct((24, plan.n[last]), f32),
        compiler_params=pltpu.CompilerParams(vmem_limit_bytes=48 << 20),
        name="coarse",
    )(ints, *recv, coarse_left)
    upper = upper[:k].reshape(k, plan.w[last], plan.r[last], plan.x[last])
    upper = jnp.pad(upper, ((0, 0), (0, 0), (0, 0), (0, LANES - plan.x[last])))

    m_fine = fine_left.shape[1]
    depth = 6 * k * SUB
    flip = planes - 1
    field, zface, yface, zfirst, sfirst = pl.pallas_call(
        fine_kernel,
        grid=(planes,),
        in_specs=[
            smem,
            whole(mid_left.shape),
            whole(fine_left.shape),
            whole(upper.shape),
            whole(noise_middle.shape),
            pl.BlockSpec((k, 1, rows, cols), lambda i: (0, flip - i, 0, 0)),
        ],
        out_specs=[
            pl.BlockSpec((2, 2 * rows, 2 * cols), lambda i: (flip - i, 0, 0)),
            pl.BlockSpec((1, 2 * rows, 2 * cols), lambda i: (flip - i, 0, 0)),
            pl.BlockSpec((2, rows, 2 * cols), lambda i: (flip - i, 0, 0)),
            whole((2 * rows, 2 * cols)),
            pl.BlockSpec((1, 2 * SUB, 2 * cols), lambda i: (flip - i, 0, 0)),
        ],
        out_shape=[
            jax.ShapeDtypeStruct((2 * planes, 2 * rows, 2 * cols), f32),
            jax.ShapeDtypeStruct((planes, 2 * rows, 2 * cols), f32),
            jax.ShapeDtypeStruct((2 * planes, rows, 2 * cols), f32),
            jax.ShapeDtypeStruct((2 * rows, 2 * cols), f32),
            jax.ShapeDtypeStruct((planes, 2 * SUB, 2 * cols), f32),
        ],
        scratch_shapes=[
            pltpu.VMEM((k, mid_planes, mid_rows, mid_cols), f32),
            pltpu.VMEM((2, mid_left.shape[1], depth), jnp.bfloat16),
            pltpu.VMEM((2, m_fine, depth), jnp.bfloat16),
            pltpu.VMEM((2 * rows, 2 * cols), f32),
        ],
        compiler_params=pltpu.CompilerParams(
            dimension_semantics=("arbitrary",), vmem_limit_bytes=52 << 20
        ),
        name="fine",
    )(
        (slab * mid_planes % 2).reshape(1).astype(jnp.int32),
        mid_left, fine_left, upper, noise_middle, noise_finest,
    )

    above = lax.ppermute(zfirst, "slab", [((i + 1) % slabs, i) for i in range(slabs)])
    edge = sfirst.reshape(2 * planes, SUB, 2 * cols)[:, SUB - 1]
    beside = lax.ppermute(edge, "pencil", [((i + 1) % pencils, i) for i in range(pencils)])
    zface = zface.at[planes - 1].add(above)
    yface = yface.at[:, rows - 1].add(beside)
    return (field, zface, yface)


def solution(mesh):
    placed = (
        P(),
        P(),
        P(),
        P(),
        P("slab", None, None),
        P(None, "slab", "pencil", None),
        P(None, "slab", "pencil", None),
    )
    return jax.shard_map(
        shards,
        mesh=mesh,
        in_specs=placed,
        out_specs=(P("slab", "pencil", None), P("slab", "pencil", None), P("slab", "pencil", None)),
        check_vma=False,
    )
```
